256 devices in a mesh: blk: 16 (over z_hi, y, core), grid: 16 (over x, z_lo).
Axes of the slice: x: 4, y: 4, z: 8 (z_hi: 2, z_lo: 4; z = z_hi * 4 + z_lo), core: 2. Of those that a mesh axis runs over, the one named last changes fastest.
Arguments:
- constraints: float32 [131072, 1024], P(('blk', 'grid')), may hold values from -0.1875 to 0.1875
- times_x: float32 [131072, 1024], P(('blk', 'grid')), may hold values from -6 to 6
- times_zinv: float32 [131072, 1024], P(('blk', 'grid')), may hold values from -6 to 6
- owner: int32 [16, 16, 16], P('blk', 'grid'), may hold values from 0 to 15, each once within a row
- update: float32 [16, 16, 16, 32, 1024], P('blk', 'grid'), may hold values from -6 to 6
Outputs:
- owned: float32 [16, 16, 16, 32, 1024], P('blk', 'grid')
The draws below stay inside these ranges and needn't reach their ends.
Inputs may be any that keep to these rules, and one draw needn't show every extreme that they name: Each owner[b, g, :] is a permutation of 0 to 15.
All inputs are finite; a program needn't handle non-finite values.
Results may differ from the reference program's by a relative error of at most 0.0003.
Values sent between devices are 32-bit elements; how exact they have to be, the bound alone decides.
A program may use at most 64 MiB of HBM per device.

```python
import jax
import jax.numpy as jnp
from jax import lax

N = 1024
ROWS = 512
ROUNDS = 2
TILE = 32
M = 131072
N_BLK = 16
N_GRID = 16


def steps_of(own_key, shape, shards, smallest, top_value):
    def one(dim, parts):
        steps = jax.random.uniform(jax.random.fold_in(jax.random.fold_in(own_key, 6), dim), (parts,), jnp.float32, smallest / len(shards), top_value / len(shards))
        return jnp.repeat(jnp.exp(steps), shape[dim] // parts).reshape((-1,) + (1,) * (len(shape) - dim - 1))

    factor_of = one(*shards[0])
    for cut in shards[1:]:
        factor_of = factor_of * one(*cut)
    return factor_of


def noise(stream_key, extent, scale, bound, split=(), kind=jnp.bfloat16):
    values = scale * jax.random.normal(stream_key, extent, jnp.float32)
    if split:
        values = values * steps_of(stream_key, extent, split, -0.22, 0.18)
    return jnp.clip(values, -bound, bound).astype(kind)


def setup_inputs(seed: int = 0) -> dict:
    seeds = jax.random.split(jax.random.key(seed), 6)
    constraints = noise(seeds[0], (M, N), N ** -0.5, 0.1875, ((0, 256),), jnp.float32)
    times_x = noise(seeds[1], (M, N), 1.0, 6.0, ((0, 256),), jnp.float32)
    times_zinv = noise(seeds[2], (M, N), 1.0, 6.0, ((0, 256),), jnp.float32)
    owner = jax.vmap(lambda own: jax.random.permutation(own, N_GRID))(jax.random.split(seeds[3], N_BLK * N_GRID)).reshape((N_BLK, N_GRID, N_GRID)).astype(jnp.int32)
    update = noise(seeds[4], (N_BLK, N_GRID, N_GRID, TILE, ROUNDS * ROWS), 1.0, 6.0, ((0, 16), (1, 16)), jnp.float32)
    return {"constraints": constraints, "times_x": times_x, "times_zinv": times_zinv, "owner": owner, "update": update}


def reference(constraints, times_x, times_zinv, owner, update):
    blocks = N_BLK * N_GRID
    tile_rows = ROWS // N_GRID
    a_blocks = constraints.reshape(blocks, ROWS, N)
    x_blocks = times_x.reshape(blocks, ROWS, N)
    z_blocks = times_zinv.reshape(blocks, ROWS, N)

    def one_block(index):
        brow = index // N_GRID
        gcol = index % N_GRID
        rows_x = lax.dynamic_index_in_dim(x_blocks, index, 0, keepdims=False)
        rows_z = lax.dynamic_index_in_dim(z_blocks, index, 0, keepdims=False)
        columns = []
        for step in range(ROUNDS):
            source = (((brow - step) % N_BLK) * N_GRID + gcol).astype(jnp.int32)
            panel = lax.dynamic_index_in_dim(a_blocks, source, 0, keepdims=False)
            left = jnp.dot(rows_x, panel.T, preferred_element_type=jnp.float32, precision=lax.Precision.HIGHEST)
            right = jnp.dot(rows_z, panel.T, preferred_element_type=jnp.float32, precision=lax.Precision.HIGHEST)
            columns.append(left * right)
        return jnp.concatenate(columns, axis=1)

    schur = lax.map(one_block, jnp.arange(blocks, dtype=jnp.int32))
    tiles = schur.reshape(N_BLK, N_GRID, N_GRID, tile_rows, ROUNDS * ROWS)
    places = jnp.arange(N_GRID, dtype=jnp.int32)
    onehot = owner[:, :, None, :] == places[None, None, :, None]
    inverse = jnp.sum(jnp.where(onehot, places[None, None, None, :], 0), axis=3).astype(jnp.int32)
    picked = jnp.take_along_axis(tiles, inverse[:, :, :, None, None], axis=2)
    return jnp.transpose(picked, (0, 2, 1, 3, 4)) - update
```

```python
import jax
import jax.numpy as jnp
from jax import lax
from jax.experimental import pallas as pl
from jax.experimental.pallas import tpu as pltpu
from jax.sharding import PartitionSpec as P

MESH = pl.DeviceIdType.MESH
ROUNDS = 2
PARTS = 4
CUTS = 4


def split(value):
    high = value.astype(jnp.bfloat16)
    return high, (value - high.astype(jnp.float32)).astype(jnp.bfloat16)


def product(left, right):
    return lax.dot_general(
        left, right, (((1,), (1,)), ((), ())), preferred_element_type=jnp.float32
    )


def kernel(
    owner_hbm, c_hbm, x_hbm, z_hbm, out,
    owner, c_own, x_own, z_own, panel, relay, c_high, c_low, lhs_high, lhs_low, send,
    load_sem, panel_send, panel_recv, relay_send, relay_recv, tile_send, tile_recv,
):
    rows, width = c_own.shape
    groups, tile_rows, _ = send.shape
    cut = rows // (PARTS * CUTS)
    blk, grid = lax.axis_index("blk"), lax.axis_index("grid")
    half, y, core = blk // 8, blk // 2 % 4, blk % 2
    x, z = grid // 4, grid % 4

    def at(half_, y_, core_):
        return (half_ * 8 + y_ * 2 + core_, grid)

    behind, ahead = ((blk + 15) % 16, grid), ((blk + 1) % 16, grid)
    other = 1 - half
    target = at(other, 0, 0)
    is_source = jnp.logical_and(core == 1, y == 3)
    is_relay = jnp.logical_and(core == 1, y < 3)
    is_target = jnp.logical_and(core == 0, y == 0)

    loads = [
        pltpu.make_async_copy(far, near, load_sem.at[i])
        for i, (far, near) in enumerate(
            ((c_hbm, c_own), (x_hbm, x_own), (z_hbm, z_own), (owner_hbm, owner))
        )
    ]
    for load in loads:
        load.start()

    barrier = pltpu.get_barrier_semaphore()

    def tell(device):
        pl.semaphore_signal(barrier, inc=1, device_id=device, device_id_type=MESH)

    for step in range(1, groups):
        tell((blk, (grid + step) % groups))
    tell(behind)

    @pl.when(is_target)
    def _():
        for part in range(PARTS - 1):
            tell(at(other, part, 1))

    @pl.when(is_relay)
    def _():
        tell(at(half, 3, 1))

    def to_panel(piece, device):
        at_rows = pl.ds(piece * cut, cut)
        return pltpu.make_async_remote_copy(
            src_ref=c_own.at[at_rows], dst_ref=panel.at[at_rows],
            send_sem=panel_send.at[piece], recv_sem=panel_recv.at[piece],
            device_id=device, device_id_type=MESH,
        )

    def to_relay(part, step):
        piece = part * CUTS + step
        return pltpu.make_async_remote_copy(
            src_ref=c_own.at[pl.ds(piece * cut, cut)], dst_ref=relay.at[step],
            send_sem=panel_send.at[piece], recv_sem=relay_recv.at[step],
            device_id=at(half, part, 1), device_id_type=MESH,
        )

    def from_relay(step):
        piece = y * CUTS + step
        return pltpu.make_async_remote_copy(
            src_ref=relay.at[step], dst_ref=panel.at[pl.ds(piece * cut, cut)],
            send_sem=relay_send.at[step], recv_sem=panel_recv.at[piece],
            device_id=target, device_id_type=MESH,
        )

    def place(j, i):
        flip_1, flip_0 = 1 - j // 2, (j + 1) // 2 % 2
        to_z = 2 * ((z // 2 + flip_1) % 2) + (z % 2 + flip_0) % 2
        return (x + i) % 4 * 4 + to_z

    def to_owner(r, h, source):
        columns = pl.ds(r * rows, rows)
        return pltpu.make_async_remote_copy(
            src_ref=send.at[h, :, columns], dst_ref=out.at[source, :, columns],
            send_sem=tile_send.at[r * groups + h], recv_sem=tile_recv.at[r * groups + source],
            device_id=(blk, h), device_id_type=MESH,
        )

    def gather(j):
        for i in range(4):
            h = place(j, i)
            t = jnp.int32(0)
            for k in range(groups):
                t = jnp.where(owner[k] == h, k, t)
            for k, rows_of in enumerate((x_own, z_own)):
                into = pl.ds((k * 4 + i) * tile_rows, tile_rows)
                high, low = split(rows_of[t])
                lhs_high[into], lhs_low[into] = high, low

    def compute(r, j):
        high, low = lhs_high[...], lhs_low[...]
        count = 4 * tile_rows
        step = 256
        for n in range(rows // step):
            at_rows = slice(n * step, (n + 1) * step)
            both = product(high, c_high[at_rows]) + product(low, c_high[at_rows])
            both = both + product(high, c_low[at_rows])
            block = both[:count] * both[count:]
            for i in range(4):
                send[place(j, i), :, r * rows + n * step : r * rows + (n + 1) * step] = block[
                    i * tile_rows : (i + 1) * tile_rows
                ]

    def ship(r, j):
        for i in range(4):
            copy = to_owner(r, place(j, i), grid)
            if i == 0:
                pl.when(j < 3)(copy.start)
            else:
                copy.start()

    def divide(values):
        for n in range(4):
            at_rows = slice(n * rows // 4, (n + 1) * rows // 4)
            c_high[at_rows], c_low[at_rows] = split(values[at_rows])

    loads[0].wait()
    divide(c_own)
    loads[1].wait()
    loads[2].wait()
    loads[3].wait()
    gather(0)

    @pl.loop(0, 4)
    def _(j):
        compute(0, j)
        gather((j + 1) % 4)

        @pl.when(j == 0)
        def _():
            extra = jnp.where(is_source, PARTS, jnp.where(is_relay, 2, 1))
            pl.semaphore_wait(barrier, groups - 1 + extra)

            @pl.when(jnp.logical_not(is_source))
            def _():
                for piece in range(PARTS * CUTS):
                    to_panel(piece, ahead).start()

            @pl.when(is_source)
            def _():
                for step in range(CUTS):
                    to_panel((PARTS - 1) * CUTS + step, target).start()
                    for part in range(PARTS - 1):
                        to_relay(part, step).start()

        ship(0, j)

    @pl.when(is_relay)
    def _():
        for step in range(CUTS):
            to_relay(0, step).wait_recv()
            from_relay(step).start()

    for piece in range(PARTS * CUTS):
        to_panel(piece, ahead).wait_recv()
    divide(panel)

    @pl.loop(0, 4)
    def _(j):
        compute(1, j)
        gather((j + 1) % 4)
        ship(1, j)

    out[grid] = send[grid]
    for piece in range(PARTS * CUTS):
        to_panel(piece, ahead).wait_send()

    @pl.when(is_relay)
    def _():
        for step in range(CUTS):
            from_relay(step).wait_send()

    for r in range(ROUNDS):

        @pl.loop(1, groups)
        def _(step):
            h = (grid + step) % groups
            copy = to_owner(r, h, h)
            copy.wait_send()
            copy.wait_recv()


def exchange(owner, constraints, times_x, times_zinv):
    rows, width = constraints.shape
    groups = owner.shape[0]
    tile_rows = rows // groups
    pieces = PARTS * CUTS
    word, half = jnp.float32, jnp.bfloat16
    hbm = pl.BlockSpec(memory_space=pltpu.HBM)
    return pl.pallas_call(
        kernel,
        out_shape=jax.ShapeDtypeStruct((groups, tile_rows, ROUNDS * rows), word),
        in_specs=[hbm] * 4,
        out_specs=pl.BlockSpec(memory_space=pltpu.VMEM),
        scratch_shapes=[
            pltpu.SMEM((groups,), jnp.int32),
            pltpu.VMEM((rows, width), word),
            pltpu.VMEM((groups, tile_rows, width), word),
            pltpu.VMEM((groups, tile_rows, width), word),
            pltpu.VMEM((rows, width), word),
            pltpu.VMEM((CUTS, rows // pieces, width), word),
            pltpu.VMEM((rows, width), half),
            pltpu.VMEM((rows, width), half),
            pltpu.VMEM((8 * tile_rows, width), half),
            pltpu.VMEM((8 * tile_rows, width), half),
            pltpu.VMEM((groups, tile_rows, ROUNDS * rows), word),
            pltpu.SemaphoreType.DMA((4,)),
            pltpu.SemaphoreType.DMA((pieces,)),
            pltpu.SemaphoreType.DMA((pieces,)),
            pltpu.SemaphoreType.DMA((CUTS,)),
            pltpu.SemaphoreType.DMA((CUTS,)),
            pltpu.SemaphoreType.DMA((ROUNDS * groups,)),
            pltpu.SemaphoreType.DMA((ROUNDS * groups,)),
        ],
        compiler_params=pltpu.CompilerParams(
            collective_id=0, has_side_effects=True, vmem_limit_bytes=32 << 20
        ),
        name="schur_exchange",
    )(
        *(
            pltpu.with_memory_space_constraint(array, pltpu.HBM)
            for array in (
                owner,
                constraints,
                times_x.reshape(groups, tile_rows, width),
                times_zinv.reshape(groups, tile_rows, width),
            )
        )
    )


def body(constraints, times_x, times_zinv, owner, update):
    joined = exchange(owner[0, 0], constraints, times_x, times_zinv)
    return joined[None, None] - update


def solution(mesh):
    placed = (
        P(("blk", "grid"), None),
        P(("blk", "grid"), None),
        P(("blk", "grid"), None),
        P("blk", "grid", None),
        P("blk", "grid", None, None, None),
    )
    return jax.shard_map(
        body,
        mesh=mesh,
        in_specs=placed,
        out_specs=P("blk", "grid", None, None, None),
        check_vma=False,
    )
```

```python
import jax
import jax.numpy as jnp
from jax import lax
from jax.experimental import pallas as pl
from jax.experimental.pallas import tpu as pltpu
from jax.sharding import PartitionSpec as P

MESH = pl.DeviceIdType.MESH
ROUNDS = 2
PARTS = 4
CUTS = 4


def split(value):
    high = value.astype(jnp.bfloat16)
    return high, (value - high.astype(jnp.float32)).astype(jnp.bfloat16)


def product(left, right):
    return lax.dot_general(
        left, right, (((1,), (1,)), ((), ())), preferred_element_type=jnp.float32
    )


def kernel(
    owner_hbm, c_hbm, x_hbm, z_hbm, update_hbm, out,
    owner, c_own, x_own, z_own, update, panel, relay, c_high, c_low, lhs_high, lhs_low, send,
    load_sem, panel_send, panel_recv, relay_send, relay_recv, tile_send, tile_recv,
):
    rows, width = c_own.shape
    groups, tile_rows, _ = send.shape
    cut = rows // (PARTS * CUTS)
    step_rows = rows // 2
    blk, grid = lax.axis_index("blk"), lax.axis_index("grid")
    half, y, core = blk // 8, blk // 2 % 4, blk % 2
    x, z = grid // 4, grid % 4

    def at(half_, y_, core_):
        return (half_ * 8 + y_ * 2 + core_, grid)

    behind, ahead = ((blk + 15) % 16, grid), ((blk + 1) % 16, grid)
    other = 1 - half
    target = at(other, 0, 0)
    is_source = jnp.logical_and(core == 1, y == 3)
    is_relay = jnp.logical_and(core == 1, y < 3)
    is_target = jnp.logical_and(core == 0, y == 0)

    first, second = pl.ds(0, rows // 2), pl.ds(rows // 2, rows // 2)
    loads = [
        pltpu.make_async_copy(far, near, load_sem.at[i])
        for i, (far, near) in enumerate(
            (
                (c_hbm.at[first], c_own.at[first]),
                (owner_hbm, owner),
                (x_hbm, x_own),
                (z_hbm, z_own),
                (c_hbm.at[second], c_own.at[second]),
                (update_hbm, update),
            )
        )
    ]
    for load in loads[:5]:
        load.start()

    barrier = pltpu.get_barrier_semaphore()

    def tell(device):
        pl.semaphore_signal(barrier, inc=1, device_id=device, device_id_type=MESH)

    for step in range(1, groups):
        tell((blk, (grid + step) % groups))
    tell(behind)

    @pl.when(is_target)
    def _():
        for part in range(PARTS - 1):
            tell(at(other, part, 1))

    @pl.when(is_relay)
    def _():
        tell(at(half, 3, 1))

    def to_panel(piece, device):
        at_rows = pl.ds(piece * cut, cut)
        return pltpu.make_async_remote_copy(
            src_ref=c_own.at[at_rows], dst_ref=panel.at[at_rows],
            send_sem=panel_send.at[piece], recv_sem=panel_recv.at[piece],
            device_id=device, device_id_type=MESH,
        )

    def to_relay(part, step):
        piece = part * CUTS + step
        return pltpu.make_async_remote_copy(
            src_ref=c_own.at[pl.ds(piece * cut, cut)], dst_ref=relay.at[step],
            send_sem=panel_send.at[piece], recv_sem=relay_recv.at[step],
            device_id=at(half, part, 1), device_id_type=MESH,
        )

    def from_relay(step):
        piece = y * CUTS + step
        return pltpu.make_async_remote_copy(
            src_ref=relay.at[step], dst_ref=panel.at[pl.ds(piece * cut, cut)],
            send_sem=relay_send.at[step], recv_sem=panel_recv.at[piece],
            device_id=target, device_id_type=MESH,
        )

    def place(j, i):
        edge = 1 - (z // 2 + z % 2) % 2
        flip_1 = (1 - j // 2) * (1 - edge) + edge * ((j + 1) // 2 % 2)
        flip_0 = (j + 1) // 2 % 2 * (1 - edge) + edge * (1 - j // 2)
        to_z = 2 * ((z // 2 + flip_1) % 2) + (z % 2 + flip_0) % 2
        return (0, 1, 3, 2)[i] * 4 + to_z

    def to_owner(r, h, source, start=0, size=None):
        columns = pl.ds(r * rows + start, size or rows)
        return pltpu.make_async_remote_copy(
            src_ref=send.at[h, :, columns], dst_ref=out.at[source, :, columns],
            send_sem=tile_send.at[r * groups + h], recv_sem=tile_recv.at[r * groups + source],
            device_id=(blk, h), device_id_type=MESH,
        )

    def gather(j):
        for i in range(4):
            h = place(j, i)
            t = jnp.int32(0)
            for k in range(groups):
                t = jnp.where(owner[k] == h, k, t)
            for k, rows_of in enumerate((x_own, z_own)):
                into = pl.ds((k * 4 + i) * tile_rows, tile_rows)
                high, low = split(rows_of[t])
                lhs_high[into], lhs_low[into] = high, low

    def compute(r, j, n):
        high, low = lhs_high[...], lhs_low[...]
        count = 4 * tile_rows
        at_rows = slice(n * step_rows, (n + 1) * step_rows)
        both = product(high, c_high[at_rows]) + product(low, c_high[at_rows])
        both = both + product(high, c_low[at_rows])
        block = both[:count] * both[count:]
        columns = slice(r * rows + n * step_rows, r * rows + (n + 1) * step_rows)
        for i in range(4):
            send[place(j, i), :, columns] = block[i * tile_rows : (i + 1) * tile_rows]

    def ship(r, j, start=0, size=None):
        for i in range(4):
            copy = to_owner(r, place(j, i), grid, start, size)
            pl.when(place(j, i) != grid)(copy.start)

    def divide(values, start, stop):
        for n in range(start, stop, 128):
            at_rows = slice(n, n + 128)
            c_high[at_rows], c_low[at_rows] = split(values[at_rows])

    loads[0].wait()
    divide(c_own, 0, rows // 2)
    for load in loads[1:4]:
        load.wait()
    gather(0)
    start = jnp.int32(0)
    compute(0, start, 0)
    loads[4].wait()
    extra = jnp.where(is_source, PARTS, jnp.where(is_relay, 2, 1))
    pl.semaphore_wait(barrier, groups - 1 + extra)

    @pl.when(jnp.logical_not(is_source))
    def _():
        for piece in range(PARTS * CUTS):
            to_panel(piece, ahead).start()

    @pl.when(is_source)
    def _():
        for step in range(CUTS):
            to_panel((PARTS - 1) * CUTS + step, target).start()
            for part in range(PARTS - 1):
                to_relay(part, step).start()

    ship(0, start, 0, step_rows)
    divide(c_own, rows // 2, rows)
    compute(0, start, 1)
    gather(1)
    ship(0, start, step_rows, rows - step_rows)
    loads[5].start()

    @pl.when(is_relay)
    def _():
        for step in range(CUTS):
            to_relay(0, step).wait_recv()
            from_relay(step).start()

    @pl.loop(1, 4)
    def _(j):
        for n in range(rows // step_rows):
            compute(0, j, n)
        gather((j + 1) % 4)
        ship(0, j)

    for piece in range(PARTS * CUTS):
        to_panel(piece, ahead).wait_recv()
    divide(panel, 0, rows)

    @pl.loop(0, 4)
    def _(j):
        for n in range(rows // step_rows):
            compute(1, j, n)
        gather((j + 1) % 4)
        ship(1, j)

    loads[5].wait()
    out[grid] = send[grid] - update[grid]
    for r in range(ROUNDS):

        @pl.loop(0, groups - 1)
        def _(step):
            h = (grid + step + 1) % groups
            columns = slice(r * rows, (r + 1) * rows)
            to_owner(r, h, h).wait_recv()
            out[h, :, columns] = out[h, :, columns] - update[h, :, columns]

    for piece in range(PARTS * CUTS):
        to_panel(piece, ahead).wait_send()

    @pl.when(is_relay)
    def _():
        for step in range(CUTS):
            from_relay(step).wait_send()

    for r in range(ROUNDS):

        @pl.loop(1, groups)
        def _(step):
            h = (grid + step) % groups
            to_owner(r, h, h).wait_send()


def exchange(owner, constraints, times_x, times_zinv, update):
    rows, width = constraints.shape
    groups = owner.shape[0]
    tile_rows = rows // groups
    pieces = PARTS * CUTS
    word, half = jnp.float32, jnp.bfloat16
    hbm = pl.BlockSpec(memory_space=pltpu.HBM)
    return pl.pallas_call(
        kernel,
        out_shape=jax.ShapeDtypeStruct((groups, tile_rows, ROUNDS * rows), word),
        in_specs=[hbm] * 5,
        out_specs=pl.BlockSpec(memory_space=pltpu.VMEM),
        scratch_shapes=[
            pltpu.SMEM((groups,), jnp.int32),
            pltpu.VMEM((rows, width), word),
            pltpu.VMEM((groups, tile_rows, width), word),
            pltpu.VMEM((groups, tile_rows, width), word),
            pltpu.VMEM((groups, tile_rows, ROUNDS * rows), word),
            pltpu.VMEM((rows, width), word),
            pltpu.VMEM((CUTS, rows // pieces, width), word),
            pltpu.VMEM((rows, width), half),
            pltpu.VMEM((rows, width), half),
            pltpu.VMEM((8 * tile_rows, width), half),
            pltpu.VMEM((8 * tile_rows, width), half),
            pltpu.VMEM((groups, tile_rows, ROUNDS * rows), word),
            pltpu.SemaphoreType.DMA((6,)),
            pltpu.SemaphoreType.DMA((pieces,)),
            pltpu.SemaphoreType.DMA((pieces,)),
            pltpu.SemaphoreType.DMA((CUTS,)),
            pltpu.SemaphoreType.DMA((CUTS,)),
            pltpu.SemaphoreType.DMA((ROUNDS * groups,)),
            pltpu.SemaphoreType.DMA((ROUNDS * groups,)),
        ],
        compiler_params=pltpu.CompilerParams(
            collective_id=0, has_side_effects=True, vmem_limit_bytes=32 << 20
        ),
        name="schur_exchange",
    )(
        *(
            pltpu.with_memory_space_constraint(array, pltpu.HBM)
            for array in (
                owner,
                constraints,
                times_x.reshape(groups, tile_rows, width),
                times_zinv.reshape(groups, tile_rows, width),
                update,
            )
        )
    )


def body(constraints, times_x, times_zinv, owner, update):
    return exchange(owner[0, 0], constraints, times_x, times_zinv, update[0, 0])[None, None]


def solution(mesh):
    placed = (
        P(("blk", "grid"), None),
        P(("blk", "grid"), None),
        P(("blk", "grid"), None),
        P("blk", "grid", None),
        P("blk", "grid", None, None, None),
    )
    return jax.shard_map(
        body,
        mesh=mesh,
        in_specs=placed,
        out_specs=P("blk", "grid", None, None, None),
        check_vma=False,
    )
```

```python
import jax
import jax.numpy as jnp
from jax import lax
from jax.experimental import pallas as pl
from jax.experimental.pallas import tpu as pltpu
from jax.sharding import PartitionSpec as P

MESH = pl.DeviceIdType.MESH
ROUNDS = 2
PARTS = 4
CUTS = 4


def split(value):
    high = value.astype(jnp.bfloat16)
    return high, (value - high.astype(jnp.float32)).astype(jnp.bfloat16)


def product(left, right):
    return lax.dot_general(
        left, right, (((1,), (1,)), ((), ())), preferred_element_type=jnp.float32
    )


def kernel(
    owner_hbm, c_hbm, x_hbm, z_hbm, update_hbm, out,
    owner, c_own, x_own, z_own, update, panel, relay, c_high, c_low, lhs_high, lhs_low, send,
    turn, load_sem, panel_send, panel_recv, relay_send, relay_recv, turn_send, turn_recv,
    tile_send, tile_recv,
):
    rows, width = c_own.shape
    groups, tile_rows, _ = send.shape
    cut = rows // (PARTS * CUTS)
    step_rows = rows // 2
    turn_rows = turn.shape[0]
    blk, grid = lax.axis_index("blk"), lax.axis_index("grid")
    half, y, core = blk // 8, blk // 2 % 4, blk % 2
    x, z = grid // 4, grid % 4

    def at(half_, y_, core_):
        return (half_ * 8 + y_ * 2 + core_, grid)

    behind, ahead = ((blk + 15) % 16, grid), ((blk + 1) % 16, grid)
    other = 1 - half
    target = at(other, 0, 0)
    is_source = jnp.logical_and(core == 1, y == 3)
    is_relay = jnp.logical_and(core == 1, y < 3)
    is_target = jnp.logical_and(core == 0, y == 0)
    edge = 1 - (z // 2 + z % 2) % 2
    is_turn = jnp.logical_and(core == 1, edge == 1)
    turned_z = (1 - half) * (1 + z // 3) + half * (3 - z)
    turn_source = (7, x * 4 + turned_z)
    turn_target = (8, x * 4 + turned_z)

    def turn_at(part):
        return (edge * 8 + part * 2 + 1, x * 4 + 3 * (1 - z % 2))


    barrier = pltpu.get_barrier_semaphore()

    def tell(device):
        pl.semaphore_signal(barrier, inc=1, device_id=device, device_id_type=MESH)

    for step in range(1, groups):
        tell((blk, (grid + step) % groups))
    tell(behind)

    @pl.when(is_target)
    def _():
        for part in range(PARTS - 1):
            tell(at(other, part, 1))

    @pl.when(is_relay)
    def _():
        tell(at(half, 3, 1))

    @pl.when(is_turn)
    def _():
        tell(turn_source)

    @pl.when(jnp.logical_and(is_target, half == 1))
    def _():
        for part in range(PARTS):
            tell(turn_at(part))

    first, second = pl.ds(0, rows // 2), pl.ds(rows // 2, rows // 2)
    loads = [
        pltpu.make_async_copy(far, near, load_sem.at[i])
        for i, (far, near) in enumerate(
            (
                (c_hbm.at[first], c_own.at[first]),
                (owner_hbm, owner),
                (x_hbm, x_own),
                (z_hbm, z_own),
                (c_hbm.at[second], c_own.at[second]),
                (update_hbm, update),
            )
        )
    ]
    for load in loads[:5]:
        load.start()

    def to_panel(piece, device, skip=0):
        at_rows = pl.ds(piece * cut + skip, cut - skip)
        return pltpu.make_async_remote_copy(
            src_ref=c_own.at[at_rows], dst_ref=panel.at[at_rows],
            send_sem=panel_send.at[piece], recv_sem=panel_recv.at[piece],
            device_id=device, device_id_type=MESH,
        )

    def to_relay(part, step, skip=0):
        piece = part * CUTS + step
        return pltpu.make_async_remote_copy(
            src_ref=c_own.at[pl.ds(piece * cut + skip, cut - skip)],
            dst_ref=relay.at[step, pl.ds(skip, cut - skip)],
            send_sem=panel_send.at[piece], recv_sem=relay_recv.at[step],
            device_id=at(half, part, 1), device_id_type=MESH,
        )

    def to_turn(part):
        return pltpu.make_async_remote_copy(
            src_ref=c_own.at[pl.ds(part * CUTS * cut, turn_rows)], dst_ref=turn,
            send_sem=panel_send.at[part * CUTS], recv_sem=turn_recv.at[0],
            device_id=turn_at(part), device_id_type=MESH,
        )

    def from_turn():
        piece = y * CUTS
        return pltpu.make_async_remote_copy(
            src_ref=turn, dst_ref=panel.at[pl.ds(piece * cut, turn_rows)],
            send_sem=turn_send.at[0], recv_sem=panel_recv.at[piece],
            device_id=turn_target, device_id_type=MESH,
        )

    def from_relay(step, skip=0):
        piece = y * CUTS + step
        return pltpu.make_async_remote_copy(
            src_ref=relay.at[step, pl.ds(skip, cut - skip)],
            dst_ref=panel.at[pl.ds(piece * cut + skip, cut - skip)],
            send_sem=relay_send.at[step], recv_sem=panel_recv.at[piece],
            device_id=target, device_id_type=MESH,
        )

    def place(j, i):
        flip_1 = (1 - j // 2) * (1 - edge) + edge * ((j + 1) // 2 % 2)
        flip_0 = (j + 1) // 2 % 2 * (1 - edge) + edge * (1 - j // 2)
        to_z = 2 * ((z // 2 + flip_1) % 2) + (z % 2 + flip_0) % 2
        return ((x + (2, 1, 3, 0)[i]) % 4) * 4 + to_z

    def to_owner(r, h, source, start=0, size=None):
        columns = pl.ds(r * rows + start, size or rows)
        return pltpu.make_async_remote_copy(
            src_ref=send.at[h, :, columns], dst_ref=out.at[source, :, columns],
            send_sem=tile_send.at[r * groups + h], recv_sem=tile_recv.at[r * groups + source],
            device_id=(blk, h), device_id_type=MESH,
        )

    def gather(j):
        for i in range(4):
            h = place(j, i)
            t = jnp.int32(0)
            for k in range(groups):
                t = jnp.where(owner[k] == h, k, t)
            for k, rows_of in enumerate((x_own, z_own)):
                into = pl.ds((k * 4 + i) * tile_rows, tile_rows)
                high, low = split(rows_of[t])
                lhs_high[into], lhs_low[into] = high, low

    def compute(r, j, n):
        high, low = lhs_high[...], lhs_low[...]
        count = 4 * tile_rows
        at_rows = slice(n * step_rows, (n + 1) * step_rows)
        both = product(high, c_high[at_rows]) + product(low, c_high[at_rows])
        both = both + product(high, c_low[at_rows])
        block = both[:count] * both[count:]
        columns = slice(r * rows + n * step_rows, r * rows + (n + 1) * step_rows)
        for i in range(4):
            send[place(j, i), :, columns] = block[i * tile_rows : (i + 1) * tile_rows]

    def ship(r, j, start=0, size=None):
        for i in range(4):
            copy = to_owner(r, place(j, i), grid, start, size)
            pl.when(place(j, i) != grid)(copy.start)

    def divide(values, start, stop):
        for n in range(start, stop, 128):
            at_rows = slice(n, n + 128)
            c_high[at_rows], c_low[at_rows] = split(values[at_rows])

    loads[0].wait()
    divide(c_own, 0, rows // 2)
    for load in loads[1:4]:
        load.wait()
    gather(0)
    start = jnp.int32(0)
    compute(0, start, 0)
    loads[4].wait()
    extra = jnp.where(is_source, PARTS, jnp.where(is_relay, 2, 1))
    extra = extra + jnp.where(jnp.logical_and(is_source, half == 0), PARTS, 0)
    extra = extra + jnp.where(is_turn, 1, 0)
    pl.semaphore_wait(barrier, groups - 1 + extra)

    @pl.when(jnp.logical_not(is_source))
    def _():
        for piece in range(PARTS * CUTS):
            to_panel(piece, ahead).start()

    @pl.when(is_source)
    def _():
        def start_first(skip):
            to_panel((PARTS - 1) * CUTS, target, skip).start()
            for part in range(PARTS - 1):
                to_relay(part, 0, skip).start()

        @pl.when(half == 0)
        def _():
            for part in range(PARTS):
                to_turn(part).start()
            start_first(turn_rows)

        @pl.when(half == 1)
        def _():
            start_first(0)

        for step in range(1, CUTS):
            to_panel((PARTS - 1) * CUTS + step, target).start()
            for part in range(PARTS - 1):
                to_relay(part, step).start()

    ship(0, start, 0, step_rows)
    divide(c_own, rows // 2, rows)
    compute(0, start, 1)
    gather(1)
    ship(0, start, step_rows, rows - step_rows)
    loads[5].start()

    @pl.when(is_relay)
    def _():
        def forward_first(skip):
            to_relay(0, 0, skip).wait_recv()
            from_relay(0, skip).start()

        @pl.when(half == 0)
        def _():
            forward_first(turn_rows)

        @pl.when(half == 1)
        def _():
            forward_first(0)

        for step in range(1, CUTS):
            to_relay(0, step).wait_recv()
            from_relay(step).start()

    @pl.when(is_turn)
    def _():
        to_turn(0).wait_recv()
        from_turn().start()

    @pl.loop(1, 4)
    def _(j):
        for n in range(rows // step_rows):
            compute(0, j, n)
        gather((j + 1) % 4)
        ship(0, j)

    for piece in range(PARTS * CUTS):
        to_panel(piece, ahead).wait_recv()
    divide(panel, 0, rows)

    @pl.loop(0, 4)
    def _(j):
        for n in range(rows // step_rows):
            compute(1, j, n)
        gather((j + 1) % 4)
        ship(1, j)

    loads[5].wait()
    out[grid] = send[grid] - update[grid]
    for r in range(ROUNDS):

        @pl.loop(0, groups - 1)
        def _(step):
            h = (grid + step + 1) % groups
            columns = slice(r * rows, (r + 1) * rows)
            to_owner(r, h, h).wait_recv()
            out[h, :, columns] = out[h, :, columns] - update[h, :, columns]

    for piece in range(PARTS * CUTS):
        to_panel(piece, ahead).wait_send()

    @pl.when(is_relay)
    def _():
        pl.when(half == 0)(from_relay(0, turn_rows).wait_send)
        pl.when(half == 1)(from_relay(0).wait_send)
        for step in range(1, CUTS):
            from_relay(step).wait_send()

    pl.when(is_turn)(from_turn().wait_send)

    for r in range(ROUNDS):

        @pl.loop(1, groups)
        def _(step):
            h = (grid + step) % groups
            to_owner(r, h, h).wait_send()


def exchange(owner, constraints, times_x, times_zinv, update):
    rows, width = constraints.shape
    groups = owner.shape[0]
    tile_rows = rows // groups
    pieces = PARTS * CUTS
    word, half = jnp.float32, jnp.bfloat16
    hbm = pl.BlockSpec(memory_space=pltpu.HBM)
    return pl.pallas_call(
        kernel,
        out_shape=jax.ShapeDtypeStruct((groups, tile_rows, ROUNDS * rows), word),
        in_specs=[hbm] * 5,
        out_specs=pl.BlockSpec(memory_space=pltpu.VMEM),
        scratch_shapes=[
            pltpu.SMEM((groups,), jnp.int32),
            pltpu.VMEM((rows, width), word),
            pltpu.VMEM((groups, tile_rows, width), word),
            pltpu.VMEM((groups, tile_rows, width), word),
            pltpu.VMEM((groups, tile_rows, ROUNDS * rows), word),
            pltpu.VMEM((rows, width), word),
            pltpu.VMEM((CUTS, rows // pieces, width), word),
            pltpu.VMEM((rows, width), half),
            pltpu.VMEM((rows, width), half),
            pltpu.VMEM((8 * tile_rows, width), half),
            pltpu.VMEM((8 * tile_rows, width), half),
            pltpu.VMEM((groups, tile_rows, ROUNDS * rows), word),
            pltpu.VMEM((rows // pieces // 2, width), word),
            pltpu.SemaphoreType.DMA((6,)),
            pltpu.SemaphoreType.DMA((pieces,)),
            pltpu.SemaphoreType.DMA((pieces,)),
            pltpu.SemaphoreType.DMA((CUTS,)),
            pltpu.SemaphoreType.DMA((CUTS,)),
            pltpu.SemaphoreType.DMA((1,)),
            pltpu.SemaphoreType.DMA((1,)),
            pltpu.SemaphoreType.DMA((ROUNDS * groups,)),
            pltpu.SemaphoreType.DMA((ROUNDS * groups,)),
        ],
        compiler_params=pltpu.CompilerParams(
            collective_id=0, has_side_effects=True, vmem_limit_bytes=32 << 20
        ),
        name="schur_exchange",
    )(
        *(
            pltpu.with_memory_space_constraint(array, pltpu.HBM)
            for array in (
                owner,
                constraints,
                times_x.reshape(groups, tile_rows, width),
                times_zinv.reshape(groups, tile_rows, width),
                update,
            )
        )
    )


def body(constraints, times_x, times_zinv, owner, update):
    return exchange(owner[0, 0], constraints, times_x, times_zinv, update[0, 0])[None, None]


def solution(mesh):
    placed = (
        P(("blk", "grid"), None),
        P(("blk", "grid"), None),
        P(("blk", "grid"), None),
        P("blk", "grid", None),
        P("blk", "grid", None, None, None),
    )
    return jax.shard_map(
        body,
        mesh=mesh,
        in_specs=placed,
        out_specs=P("blk", "grid", None, None, None),
        check_vma=False,
    )
```

```python
import jax
import jax.numpy as jnp
from jax import lax
from jax.experimental import pallas as pl
from jax.experimental.pallas import tpu as pltpu
from jax.sharding import PartitionSpec as P

MESH = pl.DeviceIdType.MESH
ROUNDS = 2
PARTS = 4
CUTS = 4


def split(value):
    high = value.astype(jnp.bfloat16)
    return high, (value - high.astype(jnp.float32)).astype(jnp.bfloat16)


def product(left, right):
    return lax.dot_general(
        left, right, (((1,), (1,)), ((), ())), preferred_element_type=jnp.float32
    )


def kernel(
    owner_hbm, c_hbm, x_hbm, z_hbm, update_hbm, out,
    owner, c_own, x_own, z_own, update, panel, relay, c_high, c_low, lhs_high, lhs_low, send,
    turn, load_sem, panel_send, panel_recv, relay_send, relay_recv, turn_send, turn_recv,
    tile_send, tile_recv,
):
    rows, width = c_own.shape
    groups, tile_rows, _ = send.shape
    cut = rows // (PARTS * CUTS)
    step_rows = rows // 2
    turn_rows = turn.shape[0]
    blk, grid = lax.axis_index("blk"), lax.axis_index("grid")
    half, y, core = blk // 8, blk // 2 % 4, blk % 2
    x, z = grid // 4, grid % 4

    def at(half_, y_, core_):
        return (half_ * 8 + y_ * 2 + core_, grid)

    behind, ahead = ((blk + 15) % 16, grid), ((blk + 1) % 16, grid)
    other = 1 - half
    target = at(other, 0, 0)
    is_source = jnp.logical_and(core == 1, y == 3)
    is_relay = jnp.logical_and(core == 1, y < 3)
    is_target = jnp.logical_and(core == 0, y == 0)
    edge = 1 - (z // 2 + z % 2) % 2
    is_turn = jnp.logical_and(core == 1, edge == 1)
    turned_z = (1 - half) * (1 + z // 3) + half * (3 - z)
    turn_source = (7, x * 4 + turned_z)
    turn_target = (8, x * 4 + turned_z)

    def turn_at(part):
        return (edge * 8 + part * 2 + 1, x * 4 + 3 * (1 - z % 2))


    barrier = pltpu.get_barrier_semaphore()

    def tell(device):
        pl.semaphore_signal(barrier, inc=1, device_id=device, device_id_type=MESH)

    for step in range(1, groups):
        tell((blk, (grid + step) % groups))
    tell(behind)

    @pl.when(is_target)
    def _():
        for part in range(PARTS - 1):
            tell(at(other, part, 1))

    @pl.when(is_relay)
    def _():
        tell(at(half, 3, 1))

    @pl.when(is_turn)
    def _():
        tell(turn_source)

    @pl.when(jnp.logical_and(is_target, half == 1))
    def _():
        for part in range(PARTS):
            tell(turn_at(part))

    first, second = pl.ds(0, rows // 2), pl.ds(rows // 2, rows // 2)
    loads = [
        pltpu.make_async_copy(far, near, load_sem.at[i])
        for i, (far, near) in enumerate(
            (
                (c_hbm.at[first], c_own.at[first]),
                (owner_hbm, owner),
                (x_hbm, x_own),
                (z_hbm, z_own),
                (c_hbm.at[second], c_own.at[second]),
                (update_hbm, update),
            )
        )
    ]
    for load in loads[:5]:
        load.start()

    def to_panel(piece, device, skip=0):
        at_rows = pl.ds(piece * cut + skip, cut - skip)
        return pltpu.make_async_remote_copy(
            src_ref=c_own.at[at_rows], dst_ref=panel.at[at_rows],
            send_sem=panel_send.at[piece], recv_sem=panel_recv.at[piece],
            device_id=device, device_id_type=MESH,
        )

    def to_relay(part, step, skip=0):
        piece = part * CUTS + step
        return pltpu.make_async_remote_copy(
            src_ref=c_own.at[pl.ds(piece * cut + skip, cut - skip)],
            dst_ref=relay.at[step, pl.ds(skip, cut - skip)],
            send_sem=panel_send.at[piece], recv_sem=relay_recv.at[step],
            device_id=at(half, part, 1), device_id_type=MESH,
        )

    def to_turn(part):
        return pltpu.make_async_remote_copy(
            src_ref=c_own.at[pl.ds(part * CUTS * cut, turn_rows)], dst_ref=turn,
            send_sem=panel_send.at[part * CUTS], recv_sem=turn_recv.at[0],
            device_id=turn_at(part), device_id_type=MESH,
        )

    def from_turn():
        piece = y * CUTS
        return pltpu.make_async_remote_copy(
            src_ref=turn, dst_ref=panel.at[pl.ds(piece * cut, turn_rows)],
            send_sem=turn_send.at[0], recv_sem=panel_recv.at[piece],
            device_id=turn_target, device_id_type=MESH,
        )

    def from_relay(step, skip=0):
        piece = y * CUTS + step
        return pltpu.make_async_remote_copy(
            src_ref=relay.at[step, pl.ds(skip, cut - skip)],
            dst_ref=panel.at[pl.ds(piece * cut + skip, cut - skip)],
            send_sem=relay_send.at[step], recv_sem=panel_recv.at[piece],
            device_id=target, device_id_type=MESH,
        )

    def place(j, i):
        flip_1 = (1 - j // 2) * (1 - edge) + edge * ((j + 1) // 2 % 2)
        flip_0 = (j + 1) // 2 % 2 * (1 - edge) + edge * (1 - j // 2)
        to_z = 2 * ((z // 2 + flip_1) % 2) + (z % 2 + flip_0) % 2
        return ((x + (2, 1, 3, 0)[i]) % 4) * 4 + to_z

    def to_owner(r, h, source, start=0, size=None):
        columns = pl.ds(r * rows + start, size or rows)
        return pltpu.make_async_remote_copy(
            src_ref=send.at[h, :, columns], dst_ref=out.at[source, :, columns],
            send_sem=tile_send.at[r * groups + h], recv_sem=tile_recv.at[r * groups + source],
            device_id=(blk, h), device_id_type=MESH,
        )

    def gather(j):
        for i in range(4):
            h = place(j, i)
            t = jnp.int32(0)
            for k in range(groups):
                t = jnp.where(owner[k] == h, k, t)
            for k, rows_of in enumerate((x_own, z_own)):
                into = pl.ds((k * 4 + i) * tile_rows, tile_rows)
                high, low = split(rows_of[t])
                lhs_high[into], lhs_low[into] = high, low

    def compute(r, j, n):
        high, low = lhs_high[...], lhs_low[...]
        count = 4 * tile_rows
        at_rows = slice(n * step_rows, (n + 1) * step_rows)
        both = product(high, c_high[at_rows]) + product(low, c_high[at_rows])
        both = both + product(high, c_low[at_rows])
        block = both[:count] * both[count:]
        columns = slice(r * rows + n * step_rows, r * rows + (n + 1) * step_rows)
        for i in range(4):
            send[place(j, i), :, columns] = block[i * tile_rows : (i + 1) * tile_rows]

    def ship(r, j, start=0, size=None):
        for i in range(4):
            copy = to_owner(r, place(j, i), grid, start, size)
            pl.when(place(j, i) != grid)(copy.start)

    def divide(values, start, stop):
        for n in range(start, stop, 128):
            at_rows = slice(n, n + 128)
            c_high[at_rows], c_low[at_rows] = split(values[at_rows])

    loads[0].wait()
    divide(c_own, 0, rows // 2)
    for load in loads[1:4]:
        load.wait()
    gather(0)
    start = jnp.int32(0)
    compute(0, start, 0)
    loads[4].wait()
    extra = jnp.where(is_source, PARTS, jnp.where(is_relay, 2, 1))
    extra = extra + jnp.where(jnp.logical_and(is_source, half == 0), PARTS, 0)
    extra = extra + jnp.where(is_turn, 1, 0)
    pl.semaphore_wait(barrier, groups - 1 + extra)

    @pl.when(jnp.logical_not(is_source))
    def _():
        for piece in range(PARTS * CUTS):
            to_panel(piece, ahead).start()

    @pl.when(is_source)
    def _():
        def start_first(skip):
            to_panel((PARTS - 1) * CUTS, target, skip).start()
            for part in range(PARTS - 1):
                to_relay(part, 0, skip).start()

        @pl.when(half == 0)
        def _():
            for part in range(PARTS):
                to_turn(part).start()
            start_first(turn_rows)

        @pl.when(half == 1)
        def _():
            start_first(0)

        for step in range(1, CUTS):
            to_panel((PARTS - 1) * CUTS + step, target).start()
            for part in range(PARTS - 1):
                to_relay(part, step).start()

    ship(0, start, 0, step_rows)
    divide(c_own, rows // 2, rows)
    compute(0, start, 1)
    gather(1)
    ship(0, start, step_rows, rows - step_rows)
    loads[5].start()

    @pl.when(is_relay)
    def _():
        def forward_first(skip):
            to_relay(0, 0, skip).wait_recv()
            from_relay(0, skip).start()

        @pl.when(half == 0)
        def _():
            forward_first(turn_rows)

        @pl.when(half == 1)
        def _():
            forward_first(0)

        for step in range(1, CUTS):
            to_relay(0, step).wait_recv()
            from_relay(step).start()

    @pl.when(is_turn)
    def _():
        to_turn(0).wait_recv()
        from_turn().start()

    @pl.loop(1, 4)
    def _(j):
        for n in range(rows // step_rows):
            compute(0, j, n)
        gather((j + 1) % 4)
        ship(0, j)

    for piece in range(PARTS * CUTS):
        to_panel(piece, ahead).wait_recv()
    divide(panel, 0, rows)

    @pl.loop(0, 4)
    def _(j):
        for n in range(rows // step_rows):
            compute(1, j, n)
        pl.when(j < 3)(lambda: gather(j + 1))
        ship(1, j)

    loads[5].wait()
    out[grid] = send[grid] - update[grid]
    for piece in range(PARTS * CUTS):
        to_panel(piece, ahead).wait_send()

    @pl.when(is_relay)
    def _():
        pl.when(half == 0)(from_relay(0, turn_rows).wait_send)
        pl.when(half == 1)(from_relay(0).wait_send)
        for step in range(1, CUTS):
            from_relay(step).wait_send()

    pl.when(is_turn)(from_turn().wait_send)

    for r in range(ROUNDS):

        @pl.loop(1, groups)
        def _(step):
            h = (grid + step) % groups
            to_owner(r, h, h).wait_send()

        @pl.loop(0, groups)
        def _(step):
            m = step // 4
            from_z = 2 * ((z // 2 + m // 2) % 2) + (z % 2 + (m + 1) // 2 % 2) % 2
            h = (x + step) % 4 * 4 + from_z
            columns = slice(r * rows, (r + 1) * rows)

            @pl.when(h != grid)
            def _():
                to_owner(r, h, h).wait_recv()
                out[h, :, columns] = out[h, :, columns] - update[h, :, columns]


def exchange(owner, constraints, times_x, times_zinv, update):
    rows, width = constraints.shape
    groups = owner.shape[0]
    tile_rows = rows // groups
    pieces = PARTS * CUTS
    word, half = jnp.float32, jnp.bfloat16
    hbm = pl.BlockSpec(memory_space=pltpu.HBM)
    return pl.pallas_call(
        kernel,
        out_shape=jax.ShapeDtypeStruct((groups, tile_rows, ROUNDS * rows), word),
        in_specs=[hbm] * 5,
        out_specs=pl.BlockSpec(memory_space=pltpu.VMEM),
        scratch_shapes=[
            pltpu.SMEM((groups,), jnp.int32),
            pltpu.VMEM((rows, width), word),
            pltpu.VMEM((groups, tile_rows, width), word),
            pltpu.VMEM((groups, tile_rows, width), word),
            pltpu.VMEM((groups, tile_rows, ROUNDS * rows), word),
            pltpu.VMEM((rows, width), word),
            pltpu.VMEM((CUTS, rows // pieces, width), word),
            pltpu.VMEM((rows, width), half),
            pltpu.VMEM((rows, width), half),
            pltpu.VMEM((8 * tile_rows, width), half),
            pltpu.VMEM((8 * tile_rows, width), half),
            pltpu.VMEM((groups, tile_rows, ROUNDS * rows), word),
            pltpu.VMEM((rows // pieces // 2, width), word),
            pltpu.SemaphoreType.DMA((6,)),
            pltpu.SemaphoreType.DMA((pieces,)),
            pltpu.SemaphoreType.DMA((pieces,)),
            pltpu.SemaphoreType.DMA((CUTS,)),
            pltpu.SemaphoreType.DMA((CUTS,)),
            pltpu.SemaphoreType.DMA((1,)),
            pltpu.SemaphoreType.DMA((1,)),
            pltpu.SemaphoreType.DMA((ROUNDS * groups,)),
            pltpu.SemaphoreType.DMA((ROUNDS * groups,)),
        ],
        compiler_params=pltpu.CompilerParams(
            collective_id=0, has_side_effects=True, vmem_limit_bytes=32 << 20
        ),
        name="schur_exchange",
    )(
        *(
            pltpu.with_memory_space_constraint(array, pltpu.HBM)
            for array in (
                owner,
                constraints,
                times_x.reshape(groups, tile_rows, width),
                times_zinv.reshape(groups, tile_rows, width),
                update,
            )
        )
    )


def body(constraints, times_x, times_zinv, owner, update):
    return exchange(owner[0, 0], constraints, times_x, times_zinv, update[0, 0])[None, None]


def solution(mesh):
    placed = (
        P(("blk", "grid"), None),
        P(("blk", "grid"), None),
        P(("blk", "grid"), None),
        P("blk", "grid", None),
        P("blk", "grid", None, None, None),
    )
    return jax.shard_map(
        body,
        mesh=mesh,
        in_specs=placed,
        out_specs=P("blk", "grid", None, None, None),
        check_vma=False,
    )
```

```python
import jax
import jax.numpy as jnp
from jax import lax
from jax.experimental import pallas as pl
from jax.experimental.pallas import tpu as pltpu
from jax.sharding import PartitionSpec as P

MESH = pl.DeviceIdType.MESH
ROUNDS = 2
PARTS = 4
CUTS = 4


def split(value):
    high = value.astype(jnp.bfloat16)
    return high, (value - high.astype(jnp.float32)).astype(jnp.bfloat16)


def product(left, right):
    return lax.dot_general(
        left, right, (((1,), (1,)), ((), ())), preferred_element_type=jnp.float32
    )


def kernel(
    owner_hbm, c_hbm, x_hbm, z_hbm, update_hbm, out,
    owner, c_own, x_own, z_own, update, panel, relay, c_high, c_low, lhs_high, lhs_low, send,
    turn, load_sem, panel_send, panel_recv, relay_send, relay_recv, turn_send, turn_recv,
    tile_send, tile_recv,
):
    rows, width = c_own.shape
    groups, tile_rows, _ = send.shape
    cut = rows // (PARTS * CUTS)
    step_rows = rows // 2
    turn_rows = turn.shape[0]
    blk, grid = lax.axis_index("blk"), lax.axis_index("grid")
    half, y, core = blk // 8, blk // 2 % 4, blk % 2
    x, z = grid // 4, grid % 4

    def at(half_, y_, core_):
        return (half_ * 8 + y_ * 2 + core_, grid)

    behind, ahead = ((blk + 15) % 16, grid), ((blk + 1) % 16, grid)
    other = 1 - half
    target = at(other, 0, 0)
    is_source = jnp.logical_and(core == 1, y == 3)
    is_relay = jnp.logical_and(core == 1, y < 3)
    is_target = jnp.logical_and(core == 0, y == 0)
    edge = 1 - (z // 2 + z % 2) % 2
    is_turn = jnp.logical_and(core == 1, edge == 1)
    turned_z = (1 - half) * (1 + z // 3) + half * (3 - z)
    turn_source = (7, x * 4 + turned_z)
    turn_target = (8, x * 4 + turned_z)

    def turn_at(part):
        return (edge * 8 + part * 2 + 1, x * 4 + 3 * (1 - z % 2))


    barrier = pltpu.get_barrier_semaphore()

    def tell(device):
        pl.semaphore_signal(barrier, inc=1, device_id=device, device_id_type=MESH)

    for step in range(1, groups):
        tell((blk, (grid + step) % groups))
    tell(behind)

    @pl.when(is_target)
    def _():
        for part in range(PARTS - 1):
            tell(at(other, part, 1))

    @pl.when(is_relay)
    def _():
        tell(at(half, 3, 1))

    @pl.when(is_turn)
    def _():
        tell(turn_source)

    @pl.when(jnp.logical_and(is_target, half == 1))
    def _():
        for part in range(PARTS):
            tell(turn_at(part))

    first, second = pl.ds(0, rows // 2), pl.ds(rows // 2, rows // 2)
    loads = [
        pltpu.make_async_copy(far, near, load_sem.at[i])
        for i, (far, near) in enumerate(
            (
                (c_hbm.at[first], c_own.at[first]),
                (owner_hbm, owner),
                (x_hbm, x_own),
                (z_hbm, z_own),
                (c_hbm.at[second], c_own.at[second]),
                (update_hbm, update),
            )
        )
    ]
    for load in loads[:5]:
        load.start()

    def to_panel(piece, device, skip=0):
        at_rows = pl.ds(piece * cut + skip, cut - skip)
        return pltpu.make_async_remote_copy(
            src_ref=c_own.at[at_rows], dst_ref=panel.at[at_rows],
            send_sem=panel_send.at[piece], recv_sem=panel_recv.at[piece],
            device_id=device, device_id_type=MESH,
        )

    def to_relay(part, step, skip=0):
        piece = part * CUTS + step
        return pltpu.make_async_remote_copy(
            src_ref=c_own.at[pl.ds(piece * cut + skip, cut - skip)],
            dst_ref=relay.at[step, pl.ds(skip, cut - skip)],
            send_sem=panel_send.at[piece], recv_sem=relay_recv.at[step],
            device_id=at(half, part, 1), device_id_type=MESH,
        )

    def to_turn(part):
        return pltpu.make_async_remote_copy(
            src_ref=c_own.at[pl.ds(part * CUTS * cut, turn_rows)], dst_ref=turn,
            send_sem=panel_send.at[part * CUTS], recv_sem=turn_recv.at[0],
            device_id=turn_at(part), device_id_type=MESH,
        )

    def from_turn():
        piece = y * CUTS
        return pltpu.make_async_remote_copy(
            src_ref=turn, dst_ref=panel.at[pl.ds(piece * cut, turn_rows)],
            send_sem=turn_send.at[0], recv_sem=panel_recv.at[piece],
            device_id=turn_target, device_id_type=MESH,
        )

    def from_relay(step, skip=0):
        piece = y * CUTS + step
        return pltpu.make_async_remote_copy(
            src_ref=relay.at[step, pl.ds(skip, cut - skip)],
            dst_ref=panel.at[pl.ds(piece * cut + skip, cut - skip)],
            send_sem=relay_send.at[step], recv_sem=panel_recv.at[piece],
            device_id=target, device_id_type=MESH,
        )

    def place(j, i):
        flip_1 = (1 - j // 2) * (1 - edge) + edge * ((j + 1) // 2 % 2)
        flip_0 = (j + 1) // 2 % 2 * (1 - edge) + edge * (1 - j // 2)
        to_z = 2 * ((z // 2 + flip_1) % 2) + (z % 2 + flip_0) % 2
        return ((x + (2, 1, 3, 0)[i]) % 4) * 4 + to_z

    def to_owner(r, h, source, start=0, size=None):
        columns = pl.ds(r * rows + start, size or rows)
        return pltpu.make_async_remote_copy(
            src_ref=send.at[h, :, columns], dst_ref=out.at[source, :, columns],
            send_sem=tile_send.at[r * groups + h], recv_sem=tile_recv.at[r * groups + source],
            device_id=(blk, h), device_id_type=MESH,
        )

    def gather(j):
        for i in range(4):
            h = place(j, i)
            t = jnp.int32(0)
            for k in range(groups):
                t = jnp.where(owner[k] == h, k, t)
            for k, rows_of in enumerate((x_own, z_own)):
                into = pl.ds((k * 4 + i) * tile_rows, tile_rows)
                high, low = split(rows_of[t])
                lhs_high[into], lhs_low[into] = high, low

    def compute(r, j, n):
        high, low = lhs_high[...], lhs_low[...]
        count = 4 * tile_rows
        at_rows = slice(n * step_rows, (n + 1) * step_rows)
        both = product(high, c_high[at_rows]) + product(low, c_high[at_rows])
        both = both + product(high, c_low[at_rows])
        block = both[:count] * both[count:]
        columns = slice(r * rows + n * step_rows, r * rows + (n + 1) * step_rows)
        for i in range(4):
            send[place(j, i), :, columns] = block[i * tile_rows : (i + 1) * tile_rows]

    def ship(r, j, start=0, size=None):
        for i in range(4):
            copy = to_owner(r, place(j, i), grid, start, size)
            pl.when(place(j, i) != grid)(copy.start)

    def divide(values, start, stop):
        for n in range(start, stop, 128):
            at_rows = slice(n, n + 128)
            c_high[at_rows], c_low[at_rows] = split(values[at_rows])

    loads[0].wait()
    divide(c_own, 0, rows // 2)
    for load in loads[1:4]:
        load.wait()
    gather(0)
    start = jnp.int32(0)
    compute(0, start, 0)
    loads[4].wait()
    extra = jnp.where(is_source, PARTS, jnp.where(is_relay, 2, 1))
    extra = extra + jnp.where(jnp.logical_and(is_source, half == 0), PARTS, 0)
    extra = extra + jnp.where(is_turn, 1, 0)
    pl.semaphore_wait(barrier, groups - 1 + extra)

    ship(0, start, 0, step_rows)

    @pl.when(jnp.logical_not(is_source))
    def _():
        for piece in range(PARTS * CUTS):
            to_panel(piece, ahead).start()

    @pl.when(is_source)
    def _():
        def start_first(skip):
            to_panel((PARTS - 1) * CUTS, target, skip).start()
            for part in range(PARTS - 1):
                to_relay(part, 0, skip).start()

        @pl.when(half == 0)
        def _():
            for part in range(PARTS):
                to_turn(part).start()
            start_first(turn_rows)

        @pl.when(half == 1)
        def _():
            start_first(0)

        for step in range(1, CUTS):
            to_panel((PARTS - 1) * CUTS + step, target).start()
            for part in range(PARTS - 1):
                to_relay(part, step).start()

    divide(c_own, rows // 2, rows)
    compute(0, start, 1)
    gather(1)
    ship(0, start, step_rows, rows - step_rows)
    loads[5].start()

    @pl.when(is_relay)
    def _():
        def forward_first(skip):
            to_relay(0, 0, skip).wait_recv()
            from_relay(0, skip).start()

        @pl.when(half == 0)
        def _():
            forward_first(turn_rows)

        @pl.when(half == 1)
        def _():
            forward_first(0)

        for step in range(1, CUTS):
            to_relay(0, step).wait_recv()
            from_relay(step).start()

    @pl.when(is_turn)
    def _():
        to_turn(0).wait_recv()
        from_turn().start()

    @pl.loop(1, 4)
    def _(j):
        for n in range(rows // step_rows):
            compute(0, j, n)
        gather((j + 1) % 4)
        ship(0, j)

    for piece in range(PARTS * CUTS):
        to_panel(piece, ahead).wait_recv()
    divide(panel, 0, rows)

    @pl.loop(0, 4)
    def _(j):
        for n in range(rows // step_rows):
            compute(1, j, n)
        pl.when(j < 3)(lambda: gather(j + 1))
        ship(1, j)

    loads[5].wait()
    out[grid] = send[grid] - update[grid]
    for piece in range(PARTS * CUTS):
        to_panel(piece, ahead).wait_send()

    @pl.when(is_relay)
    def _():
        pl.when(half == 0)(from_relay(0, turn_rows).wait_send)
        pl.when(half == 1)(from_relay(0).wait_send)
        for step in range(1, CUTS):
            from_relay(step).wait_send()

    pl.when(is_turn)(from_turn().wait_send)

    for r in range(ROUNDS):

        @pl.loop(1, groups)
        def _(step):
            h = (grid + step) % groups
            to_owner(r, h, h).wait_send()

        @pl.loop(0, groups)
        def _(step):
            m = step // 4
            from_z = 2 * ((z // 2 + m // 2) % 2) + (z % 2 + (m + 1) // 2 % 2) % 2
            h = (x + step) % 4 * 4 + from_z
            columns = slice(r * rows, (r + 1) * rows)

            @pl.when(h != grid)
            def _():
                to_owner(r, h, h).wait_recv()
                out[h, :, columns] = out[h, :, columns] - update[h, :, columns]


def exchange(owner, constraints, times_x, times_zinv, update):
    rows, width = constraints.shape
    groups = owner.shape[0]
    tile_rows = rows // groups
    pieces = PARTS * CUTS
    word, half = jnp.float32, jnp.bfloat16
    hbm = pl.BlockSpec(memory_space=pltpu.HBM)
    return pl.pallas_call(
        kernel,
        out_shape=jax.ShapeDtypeStruct((groups, tile_rows, ROUNDS * rows), word),
        in_specs=[hbm] * 5,
        out_specs=pl.BlockSpec(memory_space=pltpu.VMEM),
        scratch_shapes=[
            pltpu.SMEM((groups,), jnp.int32),
            pltpu.VMEM((rows, width), word),
            pltpu.VMEM((groups, tile_rows, width), word),
            pltpu.VMEM((groups, tile_rows, width), word),
            pltpu.VMEM((groups, tile_rows, ROUNDS * rows), word),
            pltpu.VMEM((rows, width), word),
            pltpu.VMEM((CUTS, rows // pieces, width), word),
            pltpu.VMEM((rows, width), half),
            pltpu.VMEM((rows, width), half),
            pltpu.VMEM((8 * tile_rows, width), half),
            pltpu.VMEM((8 * tile_rows, width), half),
            pltpu.VMEM((groups, tile_rows, ROUNDS * rows), word),
            pltpu.VMEM((rows // pieces // 2, width), word),
            pltpu.SemaphoreType.DMA((6,)),
            pltpu.SemaphoreType.DMA((pieces,)),
            pltpu.SemaphoreType.DMA((pieces,)),
            pltpu.SemaphoreType.DMA((CUTS,)),
            pltpu.SemaphoreType.DMA((CUTS,)),
            pltpu.SemaphoreType.DMA((1,)),
            pltpu.SemaphoreType.DMA((1,)),
            pltpu.SemaphoreType.DMA((ROUNDS * groups,)),
            pltpu.SemaphoreType.DMA((ROUNDS * groups,)),
        ],
        compiler_params=pltpu.CompilerParams(
            collective_id=0, has_side_effects=True, vmem_limit_bytes=32 << 20
        ),
        name="schur_exchange",
    )(
        *(
            pltpu.with_memory_space_constraint(array, pltpu.HBM)
            for array in (
                owner,
                constraints,
                times_x.reshape(groups, tile_rows, width),
                times_zinv.reshape(groups, tile_rows, width),
                update,
            )
        )
    )


def body(constraints, times_x, times_zinv, owner, update):
    return exchange(owner[0, 0], constraints, times_x, times_zinv, update[0, 0])[None, None]


def solution(mesh):
    placed = (
        P(("blk", "grid"), None),
        P(("blk", "grid"), None),
        P(("blk", "grid"), None),
        P("blk", "grid", None),
        P("blk", "grid", None, None, None),
    )
    return jax.shard_map(
        body,
        mesh=mesh,
        in_specs=placed,
        out_specs=P("blk", "grid", None, None, None),
        check_vma=False,
    )
```
